32 devices in a mesh: seq: 8 (over z, x), head: 4 (over y, core).
Axes of the slice: x: 2, y: 2, z: 4, core: 2. Of those that a mesh axis runs over, the one named last changes fastest.
Arguments:
- prompt_queries: bfloat16 [1536, 4096], P('seq', 'head'), may hold values from -16 to 16
- prompt_keys: bfloat16 [1536, 1024], P('seq', 'head'), may hold values from -16 to 16
- prompt_values: bfloat16 [1536, 1024], P('seq', 'head'), may hold values from -6 to 6
- span_offset: int32 [8], P('seq'), may hold values from 0 to 7, each once
- appended_queries: bfloat16 [8, 4096], P(None, 'head'), may hold values from -16 to 16
- appended_keys: bfloat16 [8, 1024], P(None, 'head'), may hold values from -6 to 6
- appended_values: bfloat16 [8, 1024], P(None, 'head'), may hold values from -6 to 6
- dec_pos: int32 [8], replicated, may hold values from 2 to 1536, as said below
- out_weight: bfloat16 [4096, 4096], P('head'), may hold values from -0.09375 to 0.09375
Outputs:
- layer_out: bfloat16 [1536, 4096], P(('seq', 'head'))
- dec_out: bfloat16 [8, 4096], P('seq', 'head')
The draws below stay inside these ranges and needn't reach their ends.
Inputs may be any that keep to these rules, and one draw needn't show every extreme that they name: span_offset is a permutation of 0 to 7. `dec_pos`: some appended token stands at 1536 in every draw.
All inputs are finite; a program needn't handle non-finite values.
Results may differ from the reference program's by a relative error of at most 0.015.
Values may be sent and summed in bfloat16 or wider, within the bound.
A program may use at most 256 MiB of HBM per device.

```python
import math
import jax
import jax.numpy as jnp
from jax import lax

D = 4096
QUERY_HEADS = 32
KEY_VALUE_HEADS = 8
HEAD_SIZE = 128
TOK_DEV = 192
PROMPT_TOKENS = 1536
APPENDED_TOKENS = 8
N_SEQ = 8


def offset_values(key, shape):
    return jnp.clip(jax.random.normal(key, shape, jnp.float32), -6.0, 6.0)


def draw_prompt_queries(key, part):
    base_offset = offset_values(jax.random.fold_in(key, 1), (PROMPT_TOKENS, QUERY_HEADS, HEAD_SIZE))
    return base_offset.reshape(PROMPT_TOKENS, QUERY_HEADS * HEAD_SIZE).astype(jnp.bfloat16)


def draw_prompt_keys(key, part):
    base_offset = offset_values(jax.random.fold_in(key, 2), (PROMPT_TOKENS, KEY_VALUE_HEADS, HEAD_SIZE))
    return base_offset.reshape(PROMPT_TOKENS, KEY_VALUE_HEADS * HEAD_SIZE).astype(jnp.bfloat16)


def draw_appended_queries(key, part):
    base_offset = offset_values(jax.random.fold_in(key, 3), (APPENDED_TOKENS, QUERY_HEADS, HEAD_SIZE))
    return base_offset.reshape(APPENDED_TOKENS, QUERY_HEADS * HEAD_SIZE).astype(jnp.bfloat16)


def draw_dec_pos(key, part):
    top_bit = max(PROMPT_TOKENS.bit_length() - 1, 1)
    powers = jax.random.randint(jax.random.fold_in(key, 4), (APPENDED_TOKENS,), 1, top_bit + 1)
    lowest = jnp.left_shift(jnp.ones((APPENDED_TOKENS,), jnp.int32), powers.astype(jnp.int32))
    extra = jax.random.randint(jax.random.fold_in(key, 5), (APPENDED_TOKENS,), 0, lowest)
    placed = jnp.minimum(lowest + extra, PROMPT_TOKENS)
    row_ids = jnp.arange(APPENDED_TOKENS, dtype=jnp.int32)
    return jnp.where(row_ids == 0, PROMPT_TOKENS, placed).astype(jnp.int32)


def level_of(rng, dims, shards, least, high):
    factor_of = 1.0
    for dim, blocks in shards:
        heights = jax.random.uniform(jax.random.fold_in(jax.random.fold_in(rng, 6), dim), (blocks,), jnp.float32, least / len(shards), high / len(shards))
        factor_of = factor_of * jnp.repeat(jnp.exp(heights), dims[dim] // blocks).reshape((-1,) + (1,) * (len(dims) - 1 - dim))
    return factor_of


def centred(rng, extent, spread, limit, cuts=(), kind=jnp.bfloat16):
    array = jax.random.normal(rng, extent, jnp.float32) * spread
    if len(cuts) > 0:
        array = level_of(rng, extent, cuts, -0.22, 0.18) * array
    return jnp.clip(array, min=-limit, max=limit).astype(kind)


def setup_inputs(seed: int = 0) -> dict:
    arg_keys = jax.random.split(jax.random.key(seed), 10)
    prompt_queries = draw_prompt_queries(jax.random.fold_in(arg_keys[9], 71), 0)
    prompt_keys = draw_prompt_keys(jax.random.fold_in(arg_keys[9], 71), 0)
    prompt_values = centred(arg_keys[2], (PROMPT_TOKENS, KEY_VALUE_HEADS * HEAD_SIZE), 1.0, 6.0, ((0, 8), (1, 4)))
    span_offset = jax.random.permutation(arg_keys[3], N_SEQ).astype(jnp.int32)
    appended_queries = draw_appended_queries(jax.random.fold_in(arg_keys[9], 71), 0)
    appended_keys = centred(arg_keys[5], (APPENDED_TOKENS, KEY_VALUE_HEADS * HEAD_SIZE), 1.0, 6.0, ((1, 4),))
    appended_values = centred(arg_keys[6], (APPENDED_TOKENS, KEY_VALUE_HEADS * HEAD_SIZE), 1.0, 6.0, ((1, 4),))
    dec_pos = draw_dec_pos(jax.random.fold_in(arg_keys[9], 71), 0)
    out_weight = centred(arg_keys[8], (QUERY_HEADS * HEAD_SIZE, D), (QUERY_HEADS * HEAD_SIZE) ** -0.5, 0.09375, ((0, 4),))
    return {"prompt_queries": prompt_queries, "prompt_keys": prompt_keys, "prompt_values": prompt_values, "span_offset": span_offset, "appended_queries": appended_queries, "appended_keys": appended_keys, "appended_values": appended_values, "dec_pos": dec_pos, "out_weight": out_weight}


masked_score = -1e30


def round_trip(values):
    return lax.optimization_barrier(values.astype(jnp.bfloat16)).astype(jnp.float32)


def reference(prompt_queries, prompt_keys, prompt_values, span_offset, appended_queries, appended_keys, appended_values, dec_pos, out_weight):
    group_width = QUERY_HEADS // KEY_VALUE_HEADS
    score_scale = HEAD_SIZE ** -0.5
    slots = jnp.arange(N_SEQ, dtype=jnp.int32)
    inverse = jnp.sum(slots[:, None] * (span_offset[:, None] == slots[None, :]).astype(jnp.int32), axis=0)

    def order_rows(matrix):
        return matrix.reshape(N_SEQ, TOK_DEV, matrix.shape[1])[inverse].reshape(PROMPT_TOKENS, matrix.shape[1])

    queries_ordered = order_rows(prompt_queries).reshape(PROMPT_TOKENS, KEY_VALUE_HEADS, group_width, HEAD_SIZE).transpose(1, 0, 2, 3).astype(jnp.float32)
    keys_ordered = order_rows(prompt_keys).reshape(PROMPT_TOKENS, KEY_VALUE_HEADS, HEAD_SIZE).transpose(1, 0, 2).astype(jnp.float32)
    values_ordered = order_rows(prompt_values).reshape(PROMPT_TOKENS, KEY_VALUE_HEADS, HEAD_SIZE).transpose(1, 0, 2).astype(jnp.float32)
    query_gradient_full = appended_queries.reshape(APPENDED_TOKENS, KEY_VALUE_HEADS, group_width, HEAD_SIZE).transpose(1, 0, 2, 3).astype(jnp.float32)
    key_gradient_full = appended_keys.reshape(APPENDED_TOKENS, KEY_VALUE_HEADS, HEAD_SIZE).transpose(1, 0, 2).astype(jnp.float32)
    value_gradient_full = appended_values.reshape(APPENDED_TOKENS, KEY_VALUE_HEADS, HEAD_SIZE).transpose(1, 0, 2).astype(jnp.float32)
    block = math.gcd(PROMPT_TOKENS, 512)
    positions = jnp.arange(PROMPT_TOKENS, dtype=jnp.int32)

    def one_group(operands):
        q_rows, k_rows, v_rows, dq_rows, dk_rows, dv_rows = operands
        pieces = []
        for number in range(PROMPT_TOKENS // block):
            begin = number * block
            finish = begin + block
            scores = jnp.einsum("rgd,sd->rgs", q_rows[begin:finish], k_rows[:finish]) * score_scale
            allowed = (positions[None, :finish] <= positions[begin:finish, None])[:, None, :]
            row_max = jnp.max(jnp.where(allowed, scores, masked_score), axis=-1, keepdims=True)
            weights = jnp.where(allowed, jnp.exp(scores - row_max), 0.0)
            denominator = jnp.sum(weights, axis=-1, keepdims=True)
            summed = jnp.einsum("rgs,sd->rgd", round_trip(weights), v_rows[:finish])
            pieces.append((summed / denominator).astype(jnp.bfloat16))
        dec_scores = jnp.einsum("rgd,sd->rgs", dq_rows, k_rows) * score_scale
        visible = (positions[None, :] < dec_pos[:, None])[:, None, :]
        self_score = jnp.einsum("rgd,rd->rg", dq_rows, dk_rows) * score_scale
        dec_max = jnp.maximum(jnp.max(jnp.where(visible, dec_scores, masked_score), axis=-1), self_score)
        dec_weights = jnp.where(visible, jnp.exp(dec_scores - dec_max[..., None]), 0.0)
        self_weight = jnp.exp(self_score - dec_max)
        dec_denominator = jnp.sum(dec_weights, axis=-1) + self_weight
        dec_summed = jnp.einsum("rgs,sd->rgd", round_trip(dec_weights), v_rows)
        dec_summed = dec_summed + round_trip(self_weight)[..., None] * dv_rows[:, None, :]
        dec_piece = (dec_summed / dec_denominator[..., None]).astype(jnp.bfloat16)
        return jnp.concatenate(pieces, axis=0), dec_piece

    prompt_attn, dec_attn = lax.map(one_group, (queries_ordered, keys_ordered, values_ordered, query_gradient_full, key_gradient_full, value_gradient_full))
    attn_sorted = prompt_attn.transpose(1, 0, 2, 3).reshape(PROMPT_TOKENS, QUERY_HEADS * HEAD_SIZE)
    attention = attn_sorted.reshape(N_SEQ, TOK_DEV, QUERY_HEADS * HEAD_SIZE)[span_offset].reshape(PROMPT_TOKENS, QUERY_HEADS * HEAD_SIZE)
    layer_out = jnp.dot(attention, out_weight, preferred_element_type=jnp.float32).astype(jnp.bfloat16)
    dec_attention = dec_attn.transpose(1, 0, 2, 3).reshape(APPENDED_TOKENS, QUERY_HEADS * HEAD_SIZE)
    dec_out = jnp.dot(dec_attention, out_weight, preferred_element_type=jnp.float32).astype(jnp.bfloat16)
    return layer_out, dec_out
```

```python
import functools
import math

import jax
import jax.numpy as jnp
from jax import lax
from jax.experimental import pallas as pl
from jax.experimental.pallas import tpu as pltpu
from jax.sharding import PartitionSpec as P

QUERY_HEADS = 32
KEY_VALUE_HEADS = 8
HEAD_SIZE = 128
GROUP = QUERY_HEADS // KEY_VALUE_HEADS
MESH = pl.DeviceIdType.MESH

masked_score = -1e30
exp2_scale = HEAD_SIZE ** (-0.5) * math.log2(math.e)


def tiled(column, width):
    return jnp.concatenate([column] * (width // column.shape[1]), axis=1)


def softmax_step(scores, allowed, value_rows, m_ref, l_ref, acc_ref, slot):
    scores = jnp.where(allowed, scores, masked_score)
    old_max = m_ref[slot]
    new_max = jnp.maximum(old_max, jnp.max(scores, axis=1, keepdims=True))
    weights = jnp.exp2((scores - tiled(new_max, scores.shape[1])) * exp2_scale)
    factor = jnp.exp2((old_max - new_max) * exp2_scale)
    m_ref[slot] = new_max
    l_ref[slot] = l_ref[slot] * factor + jnp.sum(weights, axis=1, keepdims=True)
    added = jnp.dot(
        weights.astype(jnp.bfloat16), value_rows, preferred_element_type=jnp.float32
    )
    acc_ref[slot] = acc_ref[slot] * factor + added


def kernel(
    n_seq, own_dec, chunk,
    q_ref, k_ref, v_ref, span_ref, aq_ref, ak_ref, av_ref, pos_ref, w_hbm,
    out_ref, dec_ref,
    kbuf, vbuf, obuf, wbuf, m_ref, l_ref, acc_ref, md_ref, ld_ref, accd_ref,
    attn, pbuf, own, send1, recv1, send2, recv2, dpart, dsend, drecv,
    local_sem, w_sem, ss, rs, ss1, rs1, ss2, rs2, dss, drs,
):
    tok, width = q_ref.shape
    kv_heads = k_ref.shape[1] // HEAD_SIZE
    n_dec = aq_ref.shape[0]
    model = w_hbm.shape[1]
    part = tok // 4
    line = n_seq // 2
    seq = lax.axis_index("seq")
    head = lax.axis_index("head")
    z, x = seq // 2, seq % 2
    y, c = head // 2, head % 2
    to_x = (2 * z + 1 - x, head)
    to_right = (jnp.minimum(seq + 2, n_seq - 1), head)
    to_left = (jnp.maximum(seq - 2, 0), head)
    to_core = (seq, 2 * y + 1 - c)
    to_y = (seq, 2 * (1 - y) + c)
    to_diag = (seq, 2 * (1 - y) + 1 - c)
    has_left, has_right = z > 0, z < line - 1

    weight_copy = pltpu.make_async_copy(w_hbm, wbuf, w_sem)
    weight_copy.start()
    sources = (span_ref, k_ref, v_ref)
    buffers = (obuf, kbuf, vbuf)
    locals_ = [
        pltpu.make_async_copy(sources[i], buffers[i].at[seq], local_sem.at[i]) for i in range(3)
    ]
    for copy in locals_:
        copy.start()

    barrier = pltpu.get_barrier_semaphore()
    for peer in (to_x, to_core, to_y, to_diag):
        pl.semaphore_signal(barrier, inc=1, device_id=peer, device_id_type=MESH)
    pl.when(has_left)(
        lambda: pl.semaphore_signal(barrier, inc=1, device_id=to_left, device_id_type=MESH)
    )
    pl.when(has_right)(
        lambda: pl.semaphore_signal(barrier, inc=1, device_id=to_right, device_id_type=MESH)
    )
    pl.semaphore_wait(barrier, 4 + jnp.where(has_left, 1, 0) + jnp.where(has_right, 1, 0))

    targets = (to_left, to_right, to_x)

    def moved(piece, origin, way, first=False):
        slot = buffers[piece].at[origin]
        return pltpu.make_async_remote_copy(
            src_ref=sources[piece] if first else slot,
            dst_ref=slot,
            send_sem=ss.at[way, piece, origin],
            recv_sem=rs.at[piece, origin],
            device_id=targets[way],
            device_id_type=MESH,
        )

    def nearest(j):
        reach = jnp.minimum(z, line - 1 - z)
        half = (j + 1) // 2
        both = jnp.where(j % 2 == 1, z - half, z + half)
        single = jnp.where(z < line - 1 - z, z + (j - reach), z - (j - reach))
        return jnp.where(j <= 2 * reach, both, single)

    for piece in range(3):
        pl.when(has_left)(lambda: moved(piece, seq, 0, True).start())
        pl.when(has_right)(lambda: moved(piece, seq, 1, True).start())
        moved(piece, seq, 2, True).start()

    def dec_rows(ref, h, g=0):
        col = (h * GROUP + g) * HEAD_SIZE if ref is aq_ref else h * HEAD_SIZE
        return ref[:, col : col + HEAD_SIZE].astype(jnp.float32)

    for h in range(kv_heads):
        q32 = jnp.concatenate([dec_rows(aq_ref, h, g) for g in range(GROUP)], axis=0)
        k32 = jnp.concatenate([dec_rows(ak_ref, h)] * GROUP, axis=0)
        v32 = jnp.concatenate([dec_rows(av_ref, h)] * GROUP, axis=0)
        self_score = jnp.sum(q32 * k32, axis=1, keepdims=True)
        md_ref[h] = jnp.broadcast_to(self_score, q32.shape)
        ld_ref[h] = jnp.ones(q32.shape, jnp.float32)
        accd_ref[h] = v32
    m_ref[...] = jnp.full(m_ref.shape, masked_score, jnp.float32)
    l_ref[...] = jnp.zeros(l_ref.shape, jnp.float32)
    acc_ref[...] = jnp.zeros(acc_ref.shape, jnp.float32)
    own_off = span_ref[0:1, 0:1]
    dec_index = lax.broadcasted_iota(jnp.int32, (GROUP * n_dec, 1), 0) % n_dec
    dec_limit = jnp.zeros((GROUP * n_dec, 1), jnp.int32)
    for i in range(n_dec):
        dec_limit = jnp.where(dec_index == i, pos_ref[i], dec_limit)
    for copy in locals_:
        copy.wait()

    def pair_step(j, carry):
        @pl.when(j + 1 < line)
        def _():
            zz = nearest(j + 1)
            origin = 2 * zz + x
            for piece in range(3):
                moved(piece, origin, 2).wait_recv()
                pl.when((zz < z) & has_right)(lambda: moved(piece, origin, 1).start())
                pl.when((zz > z) & has_left)(lambda: moved(piece, origin, 0).start())
                moved(piece, origin, 2).start()

        zz = nearest(j)
        for piece in range(3):
            moved(piece, 2 * zz + 1 - x, 2).wait_recv()
        key_id = lax.broadcasted_iota(jnp.int32, (1, 2 * tok), 1)
        first = key_id < tok
        offset = jnp.where(first, obuf[2 * zz][0:1, 0:1], obuf[2 * zz + 1][0:1, 0:1])
        key_pos = offset * tok + jnp.where(first, key_id, key_id - tok)
        query_pos = own_off * tok + lax.broadcasted_iota(jnp.int32, (tok, 1), 0)
        allowed = key_pos <= query_pos
        dec_allowed = key_pos < dec_limit
        for h in range(kv_heads):
            cols = slice(h * HEAD_SIZE, (h + 1) * HEAD_SIZE)
            keys = jnp.concatenate([kbuf[2 * zz, :, cols], kbuf[2 * zz + 1, :, cols]], axis=0)
            vals = jnp.concatenate([vbuf[2 * zz, :, cols], vbuf[2 * zz + 1, :, cols]], axis=0)
            for g in range(GROUP):
                i = h * GROUP + g
                queries = q_ref[:, i * HEAD_SIZE : (i + 1) * HEAD_SIZE]
                scores = lax.dot_general(
                    queries, keys, (((1,), (1,)), ((), ())),
                    preferred_element_type=jnp.float32,
                )
                softmax_step(scores, allowed, vals, m_ref, l_ref, acc_ref, i)
            q32 = jnp.concatenate([dec_rows(aq_ref, h, g) for g in range(GROUP)], axis=0)
            scores = lax.dot_general(
                q32.astype(jnp.bfloat16), keys, (((1,), (1,)), ((), ())),
                preferred_element_type=jnp.float32,
            )
            softmax_step(scores, dec_allowed, vals, md_ref, ld_ref, accd_ref, h)
        return carry

    lax.fori_loop(0, line, pair_step, 0)

    pad = attn.shape[0] - tok - n_dec
    for h in range(kv_heads):
        dec = accd_ref[h] / ld_ref[h]
        for g in range(GROUP):
            i = h * GROUP + g
            cols = slice(i * HEAD_SIZE, (i + 1) * HEAD_SIZE)
            attn[0:tok, cols] = (acc_ref[i] / l_ref[i]).astype(jnp.bfloat16)
            rows = dec[g * n_dec : (g + 1) * n_dec]
            if pad:
                rows = jnp.concatenate([rows, jnp.zeros((pad, HEAD_SIZE), jnp.float32)], axis=0)
            attn[tok:, cols] = rows.astype(jnp.bfloat16)
    weight_copy.wait()

    n_chunk = model // chunk

    def core_copy(i):
        return pltpu.make_async_remote_copy(
            src_ref=send1.at[i], dst_ref=recv1.at[i], send_sem=ss1.at[i], recv_sem=rs1.at[i],
            device_id=to_core, device_id_type=MESH,
        )

    def y_copy(i):
        return pltpu.make_async_remote_copy(
            src_ref=send2.at[i], dst_ref=recv2.at[i], send_sem=ss2.at[i], recv_sem=rs2.at[i],
            device_id=to_y, device_id_type=MESH,
        )

    def block(index):
        return pl.ds(pl.multiple_of(index * part, 8), part)

    def project(i, carry):
        @pl.when(i < n_chunk)
        def _():
            cols = pl.ds(pl.multiple_of(i * chunk, chunk), chunk)
            pbuf[...] = jnp.dot(attn[...], wbuf[:, cols], preferred_element_type=jnp.float32)
            send1[i, 0:part] = pbuf[block(2 * (1 - y) + 1 - c)].astype(jnp.bfloat16)
            send1[i, part:] = pbuf[block(2 * y + 1 - c)].astype(jnp.bfloat16)
            core_copy(i).start()
            own[i, 0:part] = pbuf[block(2 * (1 - y) + c)]
            own[i, part:] = pbuf[block(2 * y + c)]
            dpart[:, cols] = pbuf[tok : tok + n_dec]

        @pl.when(i > 0)
        def _():
            core_copy(i - 1).wait_recv()
            total = own[i - 1, 0:part] + recv1[i - 1, 0:part].astype(jnp.float32)
            send2[i - 1] = total.astype(jnp.bfloat16)
            y_copy(i - 1).start()

        return carry

    lax.fori_loop(0, n_chunk + 1, project, 0)

    quarter = model // 4
    mine = pl.ds(seq * own_dec, own_dec)

    def dec_copy(way, peer):
        return pltpu.make_async_remote_copy(
            src_ref=dsend.at[way], dst_ref=drecv.at[way],
            send_sem=dss.at[way], recv_sem=drs.at[way],
            device_id=peer, device_id_type=MESH,
        )

    dec_copies = []
    for way, peer in enumerate((to_core, to_y, to_diag)):
        cols = pl.ds(pl.multiple_of(peer[1] * quarter, 128), quarter)
        dsend[way] = dpart[mine, cols]
        dec_copies.append(dec_copy(way, peer))
        dec_copies[-1].start()

    def gather_sum(i, carry):
        y_copy(i).wait_recv()
        cols = pl.ds(pl.multiple_of(i * chunk, chunk), chunk)
        total = own[i, part:] + recv1[i, part:].astype(jnp.float32)
        out_ref[:, cols] = (total + recv2[i].astype(jnp.float32)).astype(jnp.bfloat16)
        y_copy(i).wait_send()
        core_copy(i).wait_send()
        return carry

    lax.fori_loop(0, n_chunk, gather_sum, 0)
    for copy in dec_copies:
        copy.wait()
    dec_total = dpart[mine, pl.ds(pl.multiple_of(head * quarter, 128), quarter)]
    dec_ref[...] = (dec_total + drecv[0] + drecv[1] + drecv[2]).astype(jnp.bfloat16)

    def drain(j, carry):
        zz = nearest(j)
        origin = 2 * zz + x
        for piece in range(3):
            pl.when((zz <= z) & has_right)(lambda: moved(piece, origin, 1).wait_send())
            pl.when((zz >= z) & has_left)(lambda: moved(piece, origin, 0).wait_send())
            moved(piece, origin, 2).wait_send()
        return carry

    lax.fori_loop(0, line, drain, 0)


def on_device(
    prompt_queries, prompt_keys, prompt_values, span_offset,
    appended_queries, appended_keys, appended_values, dec_pos, out_weight,
):
    n_seq = lax.axis_size("seq")
    tok, width = prompt_queries.shape
    kv_width = prompt_keys.shape[1]
    kv_heads = kv_width // HEAD_SIZE
    heads = kv_heads * GROUP
    n_dec = appended_queries.shape[0]
    own_dec = n_dec // n_seq
    model = out_weight.shape[1]
    chunk = 512
    n_chunk = model // chunk
    part = tok // 4
    rows = tok + -(-n_dec // 16) * 16
    span = jnp.broadcast_to(span_offset, (8, 128))
    vmem = pl.BlockSpec(memory_space=pltpu.VMEM)
    f32, b16 = jnp.float32, jnp.bfloat16
    dma = pltpu.SemaphoreType.DMA
    return pl.pallas_call(
        functools.partial(kernel, n_seq, own_dec, chunk),
        out_shape=(
            jax.ShapeDtypeStruct((part, model), b16),
            jax.ShapeDtypeStruct((own_dec, model // 4), b16),
        ),
        in_specs=[vmem] * 7
        + [pl.BlockSpec(memory_space=pltpu.SMEM), pl.BlockSpec(memory_space=pl.ANY)],
        out_specs=(vmem, vmem),
        scratch_shapes=[
            pltpu.VMEM((n_seq, tok, kv_width), b16),
            pltpu.VMEM((n_seq, tok, kv_width), b16),
            pltpu.VMEM((n_seq, 8, 128), jnp.int32),
            pltpu.VMEM(out_weight.shape, b16),
            pltpu.VMEM((heads, tok, HEAD_SIZE), f32),
            pltpu.VMEM((heads, tok, HEAD_SIZE), f32),
            pltpu.VMEM((heads, tok, HEAD_SIZE), f32),
            pltpu.VMEM((kv_heads, GROUP * n_dec, HEAD_SIZE), f32),
            pltpu.VMEM((kv_heads, GROUP * n_dec, HEAD_SIZE), f32),
            pltpu.VMEM((kv_heads, GROUP * n_dec, HEAD_SIZE), f32),
            pltpu.VMEM((rows, width), b16),
            pltpu.VMEM((rows, chunk), f32),
            pltpu.VMEM((n_chunk, 2 * part, chunk), f32),
            pltpu.VMEM((n_chunk, 2 * part, chunk), b16),
            pltpu.VMEM((n_chunk, 2 * part, chunk), b16),
            pltpu.VMEM((n_chunk, part, chunk), b16),
            pltpu.VMEM((n_chunk, part, chunk), b16),
            pltpu.VMEM((n_dec, model), f32),
            pltpu.VMEM((3, own_dec, model // 4), f32),
            pltpu.VMEM((3, own_dec, model // 4), f32),
            dma((3,)), dma,
            dma((3, 3, n_seq)), dma((3, n_seq)),
            dma((n_chunk,)), dma((n_chunk,)), dma((n_chunk,)), dma((n_chunk,)),
            dma((3,)), dma((3,)),
        ],
        compiler_params=pltpu.CompilerParams(
            collective_id=0, has_side_effects=True, vmem_limit_bytes=60 * 2**20
        ),
    )(
        prompt_queries, prompt_keys, prompt_values, span,
        appended_queries, appended_keys, appended_values, dec_pos, out_weight,
    )


def solution(mesh):
    in_specs = (
        P("seq", "head"),
        P("seq", "head"),
        P("seq", "head"),
        P("seq"),
        P(None, "head"),
        P(None, "head"),
        P(None, "head"),
        P(),
        P("head", None),
    )
    out_specs = (P(("seq", "head"), None), P("seq", "head"))
    return jax.shard_map(
        on_device, mesh=mesh, in_specs=in_specs, out_specs=out_specs, check_vma=False
    )
```

```python
import functools
import math

import jax
import jax.numpy as jnp
from jax import lax
from jax.experimental import pallas as pl
from jax.experimental.pallas import tpu as pltpu
from jax.sharding import PartitionSpec as P

QUERY_HEADS = 32
KEY_VALUE_HEADS = 8
HEAD_SIZE = 128
GROUP = QUERY_HEADS // KEY_VALUE_HEADS
MESH = pl.DeviceIdType.MESH

masked_score = -1e30
exp2_scale = HEAD_SIZE ** (-0.5) * math.log2(math.e)


def tiled(column, width):
    return jnp.concatenate([column] * (width // column.shape[1]), axis=1)


def softmax_step(scores, allowed, value_rows, m_ref, l_ref, acc_ref, slot):
    scores = jnp.where(allowed, scores, masked_score)
    old_max = m_ref[slot]
    new_max = jnp.maximum(old_max, jnp.max(scores, axis=1, keepdims=True))
    weights = jnp.exp2((scores - tiled(new_max, scores.shape[1])) * exp2_scale)
    factor = jnp.exp2((old_max - new_max) * exp2_scale)
    m_ref[slot] = new_max
    l_ref[slot] = l_ref[slot] * factor + jnp.sum(weights, axis=1, keepdims=True)
    added = jnp.dot(
        weights.astype(jnp.bfloat16), value_rows, preferred_element_type=jnp.float32
    )
    acc_ref[slot] = acc_ref[slot] * factor + added


def hand_on(layer_in, dec_in, layer_out, dec_out):
    layer_out[...] = layer_in[...]
    dec_out[...] = dec_in[...]


def row_cuts(tok):
    first = max(tok // 96, 1) * 16
    half = (tok - first) // 32 * 16
    return ((0, first), (first, half), (first + half, tok - first - half))


def kernel(
    n_seq, own_dec, chunk,
    q_ref, k_ref, v_ref, span_ref, aq_ref, ak_ref, av_ref, pos_ref, w_hbm,
    out_ref, dec_ref,
    kbuf, vbuf, obuf, wbuf, m_ref, l_ref, acc_ref, md_ref, ld_ref, accd_ref,
    attn, pbuf, own, send1, recv1, send2, recv2, dpart, dsend, drecv,
    local_sem, w_sem, ss, rs, ss1, rs1, ss2, rs2, dss, drs,
):
    tok, width = q_ref.shape
    kv_heads = k_ref.shape[1] // HEAD_SIZE
    n_dec = aq_ref.shape[0]
    model = w_hbm.shape[1]
    part = tok // 4
    line = n_seq // 2
    seq = lax.axis_index("seq")
    head = lax.axis_index("head")
    z, x = seq // 2, seq % 2
    y, c = head // 2, head % 2
    to_x = (2 * z + 1 - x, head)
    to_right = (jnp.minimum(seq + 2, n_seq - 1), head)
    to_left = (jnp.maximum(seq - 2, 0), head)
    to_core = (seq, 2 * y + 1 - c)
    to_y = (seq, 2 * (1 - y) + c)
    to_diag = (seq, 2 * (1 - y) + 1 - c)
    has_left, has_right = z > 0, z < line - 1

    weight_copy = pltpu.make_async_copy(w_hbm, wbuf, w_sem)
    weight_copy.start()
    cuts = row_cuts(tok)
    pieces = [(k_ref, kbuf, cuts[0]), (v_ref, vbuf, cuts[0]), (span_ref, obuf, (0, 8))]
    pieces += [(k_ref, kbuf, cut) for cut in cuts[1:]]
    pieces += [(v_ref, vbuf, cut) for cut in cuts[1:]]
    early, late = (), tuple(range(len(pieces)))
    locals_ = [
        pltpu.make_async_copy(source, buffer.at[seq], local_sem.at[i])
        for i, (source, buffer) in enumerate(
            ((span_ref, obuf), (k_ref, kbuf), (v_ref, vbuf))
        )
    ]
    for copy in locals_:
        copy.start()

    barrier = pltpu.get_barrier_semaphore()
    for peer in (to_x, to_core, to_y, to_diag):
        pl.semaphore_signal(barrier, inc=1, device_id=peer, device_id_type=MESH)
    pl.when(has_left)(
        lambda: pl.semaphore_signal(barrier, inc=1, device_id=to_left, device_id_type=MESH)
    )
    pl.when(has_right)(
        lambda: pl.semaphore_signal(barrier, inc=1, device_id=to_right, device_id_type=MESH)
    )
    pl.semaphore_wait(barrier, 4 + jnp.where(has_left, 1, 0) + jnp.where(has_right, 1, 0))

    targets = (to_left, to_right, to_x)

    def moved(piece, origin, way, first=False):
        source, buffer, (begin, size) = pieces[piece]
        slot = buffer.at[origin, pl.ds(begin, size)]
        return pltpu.make_async_remote_copy(
            src_ref=source.at[pl.ds(begin, size)] if first else slot,
            dst_ref=slot,
            send_sem=ss.at[way, piece, origin],
            recv_sem=rs.at[piece, origin],
            device_id=targets[way],
            device_id_type=MESH,
        )

    def nearest(j):
        reach = jnp.minimum(z, line - 1 - z)
        half = (j + 1) // 2
        both = jnp.where(j % 2 == 1, z - half, z + half)
        single = jnp.where(z < line - 1 - z, z + (j - reach), z - (j - reach))
        return jnp.where(j <= 2 * reach, both, single)

    partner = 2 * z + 1 - x
    for piece in early + late:
        moved(piece, seq, 2, True).start()
        pl.when(has_left)(lambda: moved(piece, seq, 0, True).start())
        pl.when(has_right)(lambda: moved(piece, seq, 1, True).start())

    def dec_rows(ref, h, g=0):
        col = (h * GROUP + g) * HEAD_SIZE if ref is aq_ref else h * HEAD_SIZE
        return ref[:, col : col + HEAD_SIZE].astype(jnp.float32)

    for h in range(kv_heads):
        q32 = jnp.concatenate([dec_rows(aq_ref, h, g) for g in range(GROUP)], axis=0)
        k32 = jnp.concatenate([dec_rows(ak_ref, h)] * GROUP, axis=0)
        v32 = jnp.concatenate([dec_rows(av_ref, h)] * GROUP, axis=0)
        self_score = jnp.sum(q32 * k32, axis=1, keepdims=True)
        md_ref[h] = jnp.broadcast_to(self_score, q32.shape)
        ld_ref[h] = jnp.ones(q32.shape, jnp.float32)
        accd_ref[h] = v32
    m_ref[...] = jnp.full(m_ref.shape, masked_score, jnp.float32)
    l_ref[...] = jnp.zeros(l_ref.shape, jnp.float32)
    acc_ref[...] = jnp.zeros(acc_ref.shape, jnp.float32)
    own_off = span_ref[0:1, 0:1]
    dec_index = lax.broadcasted_iota(jnp.int32, (GROUP * n_dec, 1), 0) % n_dec
    dec_limit = jnp.zeros((GROUP * n_dec, 1), jnp.int32)
    for i in range(n_dec):
        dec_limit = jnp.where(dec_index == i, pos_ref[i], dec_limit)
    for copy in locals_:
        copy.wait()

    for piece in early:
        moved(piece, partner, 2).wait_recv()
        pl.when(has_left)(lambda: moved(piece, partner, 0).start())
        pl.when(has_right)(lambda: moved(piece, partner, 1).start())

    arrivals = [(piece, False) for piece in early + late] + [(piece, True) for piece in early]

    def relay(distance):
        for piece, other in arrivals:
            column = 1 - x if other else x

            @pl.when(z >= distance)
            def _():
                origin = 2 * (z - distance) + column
                moved(piece, origin, 1).wait_recv()
                pl.when(has_right)(lambda: moved(piece, origin, 1).start())
                if piece in late:
                    moved(piece, origin, 2).start()

            @pl.when(z + distance < line)
            def _():
                origin = 2 * (z + distance) + column
                moved(piece, origin, 0).wait_recv()
                pl.when(has_left)(lambda: moved(piece, origin, 0).start())
                if piece in late:
                    moved(piece, origin, 2).start()

    def pair_step(j, carry):
        pl.when(j + 1 < line)(lambda: relay(j + 1))
        zz = nearest(j)
        for piece in late:
            moved(piece, 2 * zz + 1 - x, 2).wait_recv()
        key_id = lax.broadcasted_iota(jnp.int32, (1, 2 * tok), 1)
        first = key_id < tok
        offset = jnp.where(first, obuf[2 * zz][0:1, 0:1], obuf[2 * zz + 1][0:1, 0:1])
        key_pos = offset * tok + jnp.where(first, key_id, key_id - tok)
        query_pos = own_off * tok + lax.broadcasted_iota(jnp.int32, (tok, 1), 0)
        allowed = key_pos <= query_pos
        dec_allowed = key_pos < dec_limit
        for h in range(kv_heads):
            cols = slice(h * HEAD_SIZE, (h + 1) * HEAD_SIZE)
            keys = jnp.concatenate([kbuf[2 * zz, :, cols], kbuf[2 * zz + 1, :, cols]], axis=0)
            vals = jnp.concatenate([vbuf[2 * zz, :, cols], vbuf[2 * zz + 1, :, cols]], axis=0)
            for g in range(GROUP):
                i = h * GROUP + g
                queries = q_ref[:, i * HEAD_SIZE : (i + 1) * HEAD_SIZE]
                scores = lax.dot_general(
                    queries, keys, (((1,), (1,)), ((), ())),
                    preferred_element_type=jnp.float32,
                )
                softmax_step(scores, allowed, vals, m_ref, l_ref, acc_ref, i)
            q32 = jnp.concatenate([dec_rows(aq_ref, h, g) for g in range(GROUP)], axis=0)
            scores = lax.dot_general(
                q32.astype(jnp.bfloat16), keys, (((1,), (1,)), ((), ())),
                preferred_element_type=jnp.float32,
            )
            softmax_step(scores, dec_allowed, vals, md_ref, ld_ref, accd_ref, h)
        return carry

    lax.fori_loop(0, line, pair_step, 0)

    pad = attn.shape[0] - tok - n_dec
    for h in range(kv_heads):
        dec = accd_ref[h] / ld_ref[h]
        for g in range(GROUP):
            i = h * GROUP + g
            cols = slice(i * HEAD_SIZE, (i + 1) * HEAD_SIZE)
            attn[0:tok, cols] = (acc_ref[i] / l_ref[i]).astype(jnp.bfloat16)
            rows = dec[g * n_dec : (g + 1) * n_dec]
            if pad:
                rows = jnp.concatenate([rows, jnp.zeros((pad, HEAD_SIZE), jnp.float32)], axis=0)
            attn[tok:, cols] = rows.astype(jnp.bfloat16)
    weight_copy.wait()

    n_chunk = model // chunk

    def core_copy(i):
        return pltpu.make_async_remote_copy(
            src_ref=send1.at[i], dst_ref=recv1.at[i], send_sem=ss1.at[i], recv_sem=rs1.at[i],
            device_id=to_core, device_id_type=MESH,
        )

    def y_copy(i):
        return pltpu.make_async_remote_copy(
            src_ref=send2.at[i], dst_ref=recv2.at[i], send_sem=ss2.at[i], recv_sem=rs2.at[i],
            device_id=to_y, device_id_type=MESH,
        )

    def block(index):
        return pl.ds(pl.multiple_of(index * part, 8), part)

    def project(i, carry):
        @pl.when(i < n_chunk)
        def _():
            cols = pl.ds(pl.multiple_of(i * chunk, chunk), chunk)
            pbuf[...] = jnp.dot(attn[...], wbuf[:, cols], preferred_element_type=jnp.float32)
            send1[i, 0:part] = pbuf[block(2 * (1 - y) + 1 - c)].astype(jnp.bfloat16)
            send1[i, part:] = pbuf[block(2 * y + 1 - c)].astype(jnp.bfloat16)
            core_copy(i).start()
            own[i, 0:part] = pbuf[block(2 * (1 - y) + c)]
            own[i, part:] = pbuf[block(2 * y + c)]
            dpart[:, cols] = pbuf[tok : tok + n_dec]

        @pl.when(i > 0)
        def _():
            core_copy(i - 1).wait_recv()
            total = own[i - 1, 0:part] + recv1[i - 1, 0:part].astype(jnp.float32)
            send2[i - 1] = total.astype(jnp.bfloat16)
            y_copy(i - 1).start()

        return carry

    lax.fori_loop(0, n_chunk + 1, project, 0)

    quarter = model // 4
    mine = pl.ds(seq * own_dec, own_dec)

    def dec_copy(way, peer):
        return pltpu.make_async_remote_copy(
            src_ref=dsend.at[way], dst_ref=drecv.at[way],
            send_sem=dss.at[way], recv_sem=drs.at[way],
            device_id=peer, device_id_type=MESH,
        )

    dec_copies = []
    for way, peer in enumerate((to_core, to_y, to_diag)):
        cols = pl.ds(pl.multiple_of(peer[1] * quarter, 128), quarter)
        dsend[way] = dpart[mine, cols]
        dec_copies.append(dec_copy(way, peer))
        dec_copies[-1].start()

    def gather_sum(i, carry):
        y_copy(i).wait_recv()
        cols = pl.ds(pl.multiple_of(i * chunk, chunk), chunk)
        total = own[i, part:] + recv1[i, part:].astype(jnp.float32)
        out_ref[:, cols] = (total + recv2[i].astype(jnp.float32)).astype(jnp.bfloat16)
        y_copy(i).wait_send()
        core_copy(i).wait_send()
        return carry

    lax.fori_loop(0, n_chunk, gather_sum, 0)
    for copy in dec_copies:
        copy.wait()
    dec_total = dpart[mine, pl.ds(pl.multiple_of(head * quarter, 128), quarter)]
    dec_ref[...] = (dec_total + drecv[0] + drecv[1] + drecv[2]).astype(jnp.bfloat16)

    def drain(zz, carry):
        for piece, other in arrivals:
            origin = 2 * zz + (1 - x if other else x)
            pl.when((zz <= z) & has_right)(lambda: moved(piece, origin, 1).wait_send())
            pl.when((zz >= z) & has_left)(lambda: moved(piece, origin, 0).wait_send())
            if piece in late:
                moved(piece, origin, 2).wait_send()
        return carry

    for piece in early:
        moved(piece, seq, 2).wait_send()
    lax.fori_loop(0, line, drain, 0)


def on_device(
    prompt_queries, prompt_keys, prompt_values, span_offset,
    appended_queries, appended_keys, appended_values, dec_pos, out_weight,
):
    n_seq = lax.axis_size("seq")
    tok, width = prompt_queries.shape
    kv_width = prompt_keys.shape[1]
    kv_heads = kv_width // HEAD_SIZE
    heads = kv_heads * GROUP
    n_dec = appended_queries.shape[0]
    own_dec = n_dec // n_seq
    model = out_weight.shape[1]
    chunk = 512
    n_chunk = model // chunk
    part = tok // 4
    rows = tok + -(-n_dec // 16) * 16
    span = jnp.broadcast_to(span_offset, (8, 128))
    vmem = pl.BlockSpec(memory_space=pltpu.VMEM)
    f32, b16 = jnp.float32, jnp.bfloat16
    dma = pltpu.SemaphoreType.DMA
    results = pl.pallas_call(
        functools.partial(kernel, n_seq, own_dec, chunk),
        out_shape=(
            jax.ShapeDtypeStruct((part, model), b16),
            jax.ShapeDtypeStruct((own_dec, model // 4), b16),
        ),
        in_specs=[vmem] * 7
        + [pl.BlockSpec(memory_space=pltpu.SMEM), pl.BlockSpec(memory_space=pl.ANY)],
        out_specs=(vmem, vmem),
        scratch_shapes=[
            pltpu.VMEM((n_seq, tok, kv_width), b16),
            pltpu.VMEM((n_seq, tok, kv_width), b16),
            pltpu.VMEM((n_seq, 8, 128), jnp.int32),
            pltpu.VMEM(out_weight.shape, b16),
            pltpu.VMEM((heads, tok, HEAD_SIZE), f32),
            pltpu.VMEM((heads, tok, HEAD_SIZE), f32),
            pltpu.VMEM((heads, tok, HEAD_SIZE), f32),
            pltpu.VMEM((kv_heads, GROUP * n_dec, HEAD_SIZE), f32),
            pltpu.VMEM((kv_heads, GROUP * n_dec, HEAD_SIZE), f32),
            pltpu.VMEM((kv_heads, GROUP * n_dec, HEAD_SIZE), f32),
            pltpu.VMEM((rows, width), b16),
            pltpu.VMEM((rows, chunk), f32),
            pltpu.VMEM((n_chunk, 2 * part, chunk), f32),
            pltpu.VMEM((n_chunk, 2 * part, chunk), b16),
            pltpu.VMEM((n_chunk, 2 * part, chunk), b16),
            pltpu.VMEM((n_chunk, part, chunk), b16),
            pltpu.VMEM((n_chunk, part, chunk), b16),
            pltpu.VMEM((n_dec, model), f32),
            pltpu.VMEM((3, own_dec, model // 4), f32),
            pltpu.VMEM((3, own_dec, model // 4), f32),
            dma((3,)), dma,
            dma((3, 7, n_seq)), dma((7, n_seq)),
            dma((n_chunk,)), dma((n_chunk,)), dma((n_chunk,)), dma((n_chunk,)),
            dma((3,)), dma((3,)),
        ],
        compiler_params=pltpu.CompilerParams(
            collective_id=0, has_side_effects=True, vmem_limit_bytes=60 * 2**20
        ),
    )(
        prompt_queries, prompt_keys, prompt_values, span,
        appended_queries, appended_keys, appended_values, dec_pos, out_weight,
    )
    return pl.pallas_call(
        hand_on,
        out_shape=tuple(jax.ShapeDtypeStruct(r.shape, r.dtype) for r in results),
        in_specs=[vmem] * 2,
        out_specs=(vmem, vmem),
        compiler_params=pltpu.CompilerParams(vmem_limit_bytes=4 * 2**20),
    )(*results)


def solution(mesh):
    in_specs = (
        P("seq", "head"),
        P("seq", "head"),
        P("seq", "head"),
        P("seq"),
        P(None, "head"),
        P(None, "head"),
        P(None, "head"),
        P(),
        P("head", None),
    )
    out_specs = (P(("seq", "head"), None), P("seq", "head"))
    return jax.shard_map(
        on_device, mesh=mesh, in_specs=in_specs, out_specs=out_specs, check_vma=False
    )
```
